32 devices in a mesh: groups: 2 (over y), seq: 4 (over x, core), qset: 4 (over z).
Axes of the slice: x: 2, y: 2, z: 4, core: 2. Of those that a mesh axis runs over, the one named last changes fastest.
Arguments:
- states: bfloat16 [8, 4, 128, 4096], P(('groups', 'qset'), 'seq'), parts along dimension 0, may hold values from -7 to 7
- enc_gain: bfloat16 [4096], replicated, may hold values from 0.25 to 1.75
- dec_states: bfloat16 [16, 64, 4096], P(('groups', 'qset')), parts along dimension 0, may hold values from -7 to 7
- dec_gain: bfloat16 [4096], replicated, may hold values from 0.25 to 1.75
- query_weight: bfloat16 [4096, 4096], P(None, 'seq'), may hold values from -0.375 to 0.375
- key_value_weight: bfloat16 [4096, 2, 4096], P(None, None, 'seq'), may hold values from -0.0625 to 0.0625
- out_weight: bfloat16 [4096, 4096], P('seq'), may hold values from -0.75 to 0.75
- question_of: int32 [8, 4, 1], P('groups'), parts along dimension 0, may hold values from 0 to 7; in each aligned block of 4 rows (0 to 3, 4 to 7, ..., all dimensions but the last counted through in order) at most 2 rows name the same one
Outputs:
- mixed: bfloat16 [16, 64, 4096], P(('groups', 'qset'), None, 'seq'), parts along dimension 0
The draws below stay inside these ranges and needn't reach their ends.
There are 2 independent parts, one for each index of `groups`. The reference program is written for one: setup_inputs(seed, part) draws one part's arguments, and reference() takes and returns one part's arrays. A program takes and returns all parts, laid end to end along the dimension named above; an argument that names none is the same for every part. Nothing has to cross between parts.
Inputs may be any that keep to these rules, and one draw needn't show every extreme that they name: `question_of`: within each index of the first dimension (one source group of 4 passages) at most 2 passages name the same question, and exactly 2 do for some question in some groups; every question is named by at least one passage.
All inputs are finite; a program needn't handle non-finite values.
Results may differ from the reference program's by a relative error of at most 0.014.
The reference program's roundings to bfloat16 on the way count: a program that leaves them out, or rounds other values in their place, can miss the bound.
Values may be sent and summed in bfloat16 or wider, within the bound.
No kernel may reach another device: no remote copies, remote signals or barrier semaphores. Data moves between devices by JAX's collectives and lax.ppermute only.
A program may use at most 128 MiB of HBM per device.

```python
import math
import jax
import jax.numpy as jnp
import numpy as np
from jax import lax

D = 4096
HEADS = 64
HD = 64
PLEN = 128
CAP = 2
DTOK = 64
QUESTIONS = 8
N_SEQ = 4
N_QSET = 4


def drawn_rows(salt_key, lead_shape):
    values = jax.random.normal(jax.random.fold_in(salt_key, 105), lead_shape + (D,), jnp.float32)
    return jnp.clip(values, -6.0, 6.0)


def draw_states(key, part):
    salt_key = jax.random.fold_in(key, 11)
    lead_shape = (N_QSET, N_SEQ, PLEN)
    result = drawn_rows(salt_key, lead_shape)
    return result.astype(jnp.bfloat16)


def draw_dec_states(key, part):
    salt_key = jax.random.fold_in(key, 12)
    lead_shape = (QUESTIONS, DTOK)
    result = drawn_rows(salt_key, lead_shape)
    return result.astype(jnp.bfloat16)


def weight_tables(key):
    key_part = jax.random.normal(jax.random.fold_in(key, 201), (D, 2, HEADS * HD), jnp.float32)
    key_part = jnp.clip(key_part, -4.0, 4.0) * D ** (-0.5)
    query_part = jax.random.normal(jax.random.fold_in(key, 202), (D, HEADS * HD), jnp.float32)
    query_part = jnp.clip(query_part, -4.0, 4.0) * (D * HD) ** (-0.5)
    return (key_part, query_part)


def draw_key_value_weight(key, part):
    key_part, query_part = weight_tables(key)
    return key_part.astype(jnp.bfloat16)


def draw_query_weight(key, part):
    key_part, query_part = weight_tables(key)
    result = query_part
    return result.astype(jnp.bfloat16)


def steps_of(own_key, dims, split, low, largest):
    def one(dim, blocks):
        draws = jax.random.uniform(jax.random.fold_in(jax.random.fold_in(own_key, 6), dim), (blocks,), jnp.float32, low / len(split), largest / len(split))
        return jnp.repeat(jnp.exp(draws), dims[dim] // blocks).reshape((-1,) + (1,) * (len(dims) - dim - 1))

    loudness = one(*split[0])
    for cut in split[1:]:
        loudness = loudness * one(*cut)
    return loudness


def shared_out(rng, own, number, rows, amount, top, bound, slope):
    order = jax.random.permutation(rng, amount)
    heavy_load, ordinary = load_shares(amount, rows * top, bound, slope, True), load_shares(amount, rows * top, bound, slope, False)
    places = jnp.arange(amount)

    def named(tallies, offset_by):
        used = int((tallies > 0).sum())
        fixed = max(1, used // 4)
        shifted = fixed + (places - fixed + offset_by * (used - fixed)) % max(1, amount - fixed)
        return jnp.zeros((amount,), jnp.int32).at[order[jnp.where(places < fixed, places, shifted)]].set(jnp.asarray(tallies, jnp.int32))

    tallies = jnp.where(number % 4 == 0, named(heavy_load, number // 4), named(ordinary, number - number // 4 - 1))
    mixed = jax.random.permutation(jax.random.fold_in(own, 3), amount)
    giver, sink = mixed[0:amount // 2 * 2:2], mixed[1:amount // 2 * 2:2]
    room = jnp.minimum(tallies[giver] - 1, bound - tallies[sink]) // 2
    room = jnp.where((giver == order[0]) | (sink == order[0]) | (tallies[sink] == 0), 0, jnp.maximum(room, 0))
    shifted = jax.random.randint(jax.random.fold_in(own, 4), (amount // 2,), 0, 1 << 20) % (room + 1)
    tallies = tallies.at[giver].add(-shifted).at[sink].add(shifted)
    items = jnp.searchsorted(jnp.cumsum(tallies), jnp.arange(rows * top), side="right").astype(jnp.int32)
    table = items.reshape(top, rows).T
    table = table[jax.random.permutation(jax.random.fold_in(own, 1), rows)]
    offset_by = jax.random.randint(jax.random.fold_in(own, 2), (rows, 1), 0, top)
    return jnp.take_along_axis(table, (jnp.arange(top)[None, :] + offset_by) % top, axis=1)


def load_shares(amount, total, reach, skew, full):
    portions = [(1 << 20) // math.isqrt(rank ** skew) + 1 for rank in range(1, amount + 1)]
    largest = reach if full else min(reach, max(-(-total // amount), total * portions[0] // sum(portions)))
    least = 1 if total - largest >= amount - 1 else 0
    given, surplus = [largest] + [least] * (amount - 1), total - largest - least * (amount - 1)
    while surplus > 0:
        movable = [i for i in range(1, amount) if given[i] < largest] or [i for i in range(1, amount) if given[i] < reach]
        whole, budget = sum([portions[i] for i in movable]), surplus
        for i in movable:
            more = min(reach - given[i], max(1, budget * portions[i] // whole), surplus)
            given[i] = given[i] + more
            surplus = surplus - more
    return np.array(given)


def normal_values(rng, shape, width, limit, split=(), held_as=jnp.bfloat16):
    array = jax.random.normal(rng, shape, jnp.float32) * width
    if len(split) > 0:
        array = steps_of(rng, shape, split, -0.22, 0.18) * array
    return jnp.clip(array, min=-limit, max=limit).astype(held_as)


def setup_inputs(seed: int = 0, part: int = 0) -> dict:
    arg_keys = jax.random.split(jax.random.key(seed), 9)
    part_keys = jax.random.split(jax.random.fold_in(arg_keys[8], part), 9)
    states = draw_states(jax.random.fold_in(jax.random.fold_in(arg_keys[8], part), 71), part)
    enc_gain = jnp.clip(1.0 + 0.15 * jax.random.normal(arg_keys[1], (D,), jnp.float32), 0.25, 1.75).astype(jnp.bfloat16)
    dec_states = draw_dec_states(jax.random.fold_in(jax.random.fold_in(arg_keys[8], part), 71), part)
    dec_gain = jnp.clip(1.0 + 0.15 * jax.random.normal(arg_keys[3], (D,), jnp.float32), 0.25, 1.75).astype(jnp.bfloat16)
    query_weight = draw_query_weight(jax.random.fold_in(arg_keys[8], 71), part)
    key_value_weight = draw_key_value_weight(jax.random.fold_in(arg_keys[8], 71), part)
    out_weight = normal_values(arg_keys[6], (HEADS * HD, D), HD ** -0.5, 0.75, ((0, 4),))
    question_of_keys = jax.random.split(jax.random.fold_in(part_keys[7], 1), N_QSET * N_SEQ // N_SEQ)
    question_of_turns = jax.random.permutation(jax.random.fold_in(part_keys[7], 3), N_QSET * N_SEQ // N_SEQ)
    question_of = jax.vmap(lambda own, number: shared_out(jax.random.fold_in(part_keys[7], 2), own, number, N_SEQ, QUESTIONS, 1, CAP, 2))(question_of_keys, question_of_turns).reshape((N_QSET, N_SEQ, 1))
    return {"states": states, "enc_gain": enc_gain, "dec_states": dec_states, "dec_gain": dec_gain, "query_weight": query_weight, "key_value_weight": key_value_weight, "out_weight": out_weight, "question_of": question_of}


EPSILON = 1e-06
MASKED_SCORE = -1e+30

def scaled_norm(rows_in, gain_vec):
    rows_f32 = rows_in.astype(jnp.float32)
    mean_square = lax.optimization_barrier(jnp.mean(rows_f32 * rows_f32, axis=-1, keepdims=True))
    return rows_f32 * lax.rsqrt(mean_square + EPSILON) * gain_vec.astype(jnp.float32)

def rounded(values_in):
    return lax.optimization_barrier(values_in.astype(jnp.bfloat16)).astype(jnp.float32)

def reference(states, enc_gain, dec_states, dec_gain, query_weight, key_value_weight, out_weight, question_of):
    enc_rows = scaled_norm(states, enc_gain).astype(jnp.bfloat16).reshape(-1, D)
    passage_question = question_of.reshape(-1).astype(jnp.int32)
    row_question = jnp.repeat(passage_question, PLEN)
    question_count = dec_states.shape[0]
    live_mask = row_question[None, :] == jnp.arange(question_count, dtype=jnp.int32)[:, None]
    dec_rows = scaled_norm(dec_states, dec_gain).astype(jnp.bfloat16).reshape(-1, D)
    query_heads = jnp.transpose(query_weight.reshape(D, HEADS, HD), (1, 0, 2))
    key_heads = jnp.transpose(key_value_weight[:, 0, :].reshape(D, HEADS, HD), (1, 0, 2))
    value_heads = jnp.transpose(key_value_weight[:, 1, :].reshape(D, HEADS, HD), (1, 0, 2))
    out_heads = out_weight.reshape(HEADS, HD, D)

    def one_head(carry, weights_in):
        w_query, w_key, w_value, w_out = weights_in
        queries = jnp.dot(dec_rows, w_query, preferred_element_type=jnp.float32).astype(jnp.bfloat16)
        key_rows = jnp.dot(enc_rows, w_key, preferred_element_type=jnp.float32).astype(jnp.bfloat16)
        value_rows = jnp.dot(enc_rows, w_value, preferred_element_type=jnp.float32).astype(jnp.bfloat16)
        query_blocks = rounded(queries).reshape(question_count, -1, HD)
        scores = jnp.einsum('qtd,rd->qtr', query_blocks, key_rows.astype(jnp.float32))
        scores = jnp.where(live_mask[:, None, :], scores, MASKED_SCORE)
        row_peak = lax.optimization_barrier(jnp.max(scores, axis=-1, keepdims=True))
        weights = jnp.where(live_mask[:, None, :], jnp.exp(scores - row_peak), 0.0)
        row_total = lax.optimization_barrier(jnp.sum(weights, axis=-1, keepdims=True))
        summed = jnp.einsum('qtr,rd->qtd', rounded(weights), value_rows.astype(jnp.float32))
        attended = (summed / row_total).astype(jnp.bfloat16).reshape(-1, HD)
        return (carry + jnp.dot(attended, w_out, preferred_element_type=jnp.float32), None)
    start_sum = jnp.zeros((dec_rows.shape[0], D), jnp.float32)
    projected, unused = lax.scan(one_head, start_sum, (query_heads, key_heads, value_heads, out_heads))
    mixed = dec_states.astype(jnp.float32) + projected.reshape(dec_states.shape)
    return mixed.astype(jnp.bfloat16)
```

```python
import functools

import jax
import jax.numpy as jnp
from jax import lax
from jax.experimental import pallas as pl
from jax.experimental.pallas import tpu as pltpu
from jax.sharding import PartitionSpec as P

HD = 64
EPSILON = 1e-06
EMPTY = -1e30
LANES = 128
CHUNKS = 4


F32 = jnp.float32
BF16 = jnp.bfloat16


def cost(flops, bytes_accessed):
    return pl.CostEstimate(flops=int(flops), bytes_accessed=int(bytes_accessed), transcendentals=0)


def full_spec():
    return pl.BlockSpec(memory_space=pltpu.VMEM)


def enc_norm_kernel(x_ref, g_ref, *out_refs):
    x = x_ref[...].astype(F32)
    scale = lax.rsqrt(jnp.mean(x * x, axis=-1, keepdims=True) + EPSILON)
    width = out_refs[0].shape[1]
    for i, out in enumerate(out_refs):
        cols = slice(i * width, (i + 1) * width)
        out[...] = (x_ref[:, cols].astype(F32) * scale * g_ref[:, cols].astype(F32)).astype(BF16)


def enc_norm(x, gain):
    rows, width = x.shape
    piece = width // CHUNKS
    return pl.pallas_call(
        enc_norm_kernel,
        in_specs=[full_spec(), full_spec()],
        out_specs=[full_spec()] * CHUNKS,
        out_shape=[jax.ShapeDtypeStruct((rows, piece), BF16)] * CHUNKS,
        cost_estimate=cost(rows * width * 8, rows * width * 4),
        name="enc_norm",
    )(x, gain)


def query_kernel(x_ref, g_ref, w_ref, out_ref, rows_ref):
    @pl.when(pl.program_id(0) == 0)
    def _():
        x = x_ref[...].astype(F32)
        scale = lax.rsqrt(jnp.mean(x * x, axis=-1, keepdims=True) + EPSILON)
        rows_ref[...] = (x * scale * g_ref[...].astype(F32)).astype(BF16)

    out_ref[...] = jnp.dot(rows_ref[...], w_ref[...], preferred_element_type=F32).astype(BF16)


def query_rows(x, gain, weight):
    rows, width = x.shape
    cols = weight.shape[1]
    tile = min(256, cols)
    return pl.pallas_call(
        query_kernel,
        grid=(cols // tile,),
        in_specs=[
            pl.BlockSpec((rows, width), lambda i: (0, 0)),
            pl.BlockSpec((1, width), lambda i: (0, 0)),
            pl.BlockSpec((width, tile), lambda i: (0, i)),
        ],
        out_specs=pl.BlockSpec((rows, tile), lambda i: (0, i)),
        out_shape=jax.ShapeDtypeStruct((rows, cols), BF16),
        scratch_shapes=[pltpu.VMEM((rows, width), BF16)],
        cost_estimate=cost(2 * rows * width * cols, width * cols * 2),
        name="query_rows",
    )(x, gain, weight)


def split3(x):
    hi = x.astype(BF16)
    rest = x - hi.astype(F32)
    mid = rest.astype(BF16)
    low = (rest - mid.astype(F32)).astype(BF16)
    return hi, mid, low


def attend_kernel(n_pass, plen, heads, dests, table, *refs):
    q_refs = refs[:dests]
    kv_ref = refs[dests]
    out_refs = refs[dests + 1 : 2 * dests + 1]
    qs, part, peak_s, total_s = refs[2 * dests + 1 :]
    per, dec_len, cols = out_refs[0].shape[0], out_refs[0].shape[1], heads * HD
    pairs = cols // LANES
    for i, ref in enumerate(q_refs):
        for j in range(per):
            qs[i * per + j] = ref[j * dec_len : (j + 1) * dec_len, :]
    lane = lax.broadcasted_iota(jnp.int32, (dec_len, LANES), 1)
    left = lane < HD

    def one_passage(p, carry):
        slot = table[0, p]
        first = pl.multiple_of(p * plen, plen)
        peaks = jnp.zeros((dec_len, LANES), F32)
        totals = jnp.zeros((dec_len, LANES), F32)
        for b in range(pairs):
            span = slice(b * LANES, (b + 1) * LANES)
            q = qs[slot, :, span]
            zero = jnp.zeros_like(q)
            both = jnp.concatenate([jnp.where(left, q, zero), jnp.where(left, zero, q)], axis=0)
            scores = lax.dot_general(
                both,
                kv_ref[0, pl.ds(first, plen), span],
                (((1,), (1,)), ((), ())),
                preferred_element_type=F32,
            )
            peak = jnp.max(scores, axis=-1, keepdims=True)
            weights = jnp.exp(scores - peak)
            total = jnp.sum(weights, axis=-1, keepdims=True)
            summed = jnp.dot(
                weights.astype(BF16),
                kv_ref[1, pl.ds(first, plen), span],
                preferred_element_type=F32,
            )
            summed = summed / total
            part[p, :, span] = jnp.where(left, summed[:dec_len], summed[dec_len:])
            for side in range(2):
                here = lane == 2 * b + side
                rows = slice(side * dec_len, (side + 1) * dec_len)
                peaks = jnp.where(here, peak[rows], peaks)
                totals = jnp.where(here, total[rows], totals)
        peak_s[p] = peaks
        total_s[p] = totals
        return carry

    lax.fori_loop(0, n_pass, one_passage, 0)

    def put_stats(out, j, peaks, totals):
        p_hi, p_mid, p_low = split3(peaks)
        t_hi, t_low, _ = split3(totals)
        packed = jnp.concatenate(
            [v[:, :heads] for v in (p_hi, p_mid, p_low, t_hi, t_low)]
            + [jnp.zeros((dec_len, LANES - 5 * heads), BF16)],
            axis=1,
        )
        out[j, :, cols:] = packed

    for r, out in enumerate(out_refs):
        for j in range(per):
            t = r * per + j
            a, b = table[1, t], table[2, t]

            @pl.when(a < 0)
            def _():
                out[j, :, :cols] = jnp.zeros((dec_len, cols), BF16)
                put_stats(
                    out, j, jnp.full((dec_len, LANES), EMPTY, F32), jnp.zeros((dec_len, LANES), F32)
                )

            @pl.when((a >= 0) & (b < 0))
            def _():
                out[j, :, :cols] = part[a].astype(BF16)
                put_stats(out, j, peak_s[a], total_s[a])

            @pl.when((a >= 0) & (b >= 0))
            def _():
                peaks = jnp.maximum(peak_s[a], peak_s[b])
                size_a = total_s[a] * jnp.exp(peak_s[a] - peaks)
                size_b = total_s[b] * jnp.exp(peak_s[b] - peaks)
                totals = size_a + size_b
                totals_safe = jnp.where(totals > 0, totals, 1.0)
                w_a, w_b = size_a / totals_safe, size_b / totals_safe
                for c in range(pairs):
                    span = slice(c * LANES, (c + 1) * LANES)
                    fa = jnp.where(left, w_a[:, 2 * c : 2 * c + 1], w_a[:, 2 * c + 1 : 2 * c + 2])
                    fb = jnp.where(left, w_b[:, 2 * c : 2 * c + 1], w_b[:, 2 * c + 1 : 2 * c + 2])
                    out[j, :, span] = (part[a, :, span] * fa + part[b, :, span] * fb).astype(BF16)
                put_stats(out, j, peaks, totals)


def attend(table, queries, kv, n_pass, plen, per, dec_len):
    dests = len(queries)
    cols = queries[0].shape[1]
    heads = cols // HD
    rows = n_pass * dec_len
    return pl.pallas_call(
        functools.partial(attend_kernel, n_pass, plen, heads, dests),
        in_specs=[pl.BlockSpec(memory_space=pltpu.SMEM)] + [full_spec()] * (dests + 1),
        out_specs=[full_spec()] * dests,
        out_shape=[jax.ShapeDtypeStruct((per, dec_len, cols + LANES), BF16)] * dests,
        scratch_shapes=[
            pltpu.VMEM((dests * per, dec_len, cols), BF16),
            pltpu.VMEM((n_pass, dec_len, cols), F32),
            pltpu.VMEM((n_pass, dec_len, LANES), F32),
            pltpu.VMEM((n_pass, dec_len, LANES), F32),
        ],
        cost_estimate=cost(8 * rows * plen * cols, n_pass * plen * cols * 4),
        name="attend",
    )(table, *queries, kv)


def project_kernel(heads, parts, order, *refs):
    part_refs = refs[:parts]
    w_ref = refs[parts]
    out_ref, rows_ref = refs[parts + 1 :]
    per, dec_len = part_refs[0].shape[0], part_refs[0].shape[1]
    cols = heads * HD

    @pl.when(pl.program_id(0) == 0)
    def _():
        lane = lax.broadcasted_iota(jnp.int32, (dec_len, LANES), 1)
        left = lane < HD
        for j in range(per):
            peaks, totals = [], []
            for ref in part_refs:
                stats = ref[j, :, cols:].astype(F32)
                cut = [stats[:, i * heads : (i + 1) * heads] for i in range(5)]
                peaks.append(cut[0] + cut[1] + cut[2])
                totals.append(cut[3] + cut[4])
            top = functools.reduce(jnp.maximum, peaks)
            sizes = [t * jnp.exp(p - top) for p, t in zip(peaks, totals)]
            whole = functools.reduce(jnp.add, sizes)
            shares = [s / whole for s in sizes]
            for c in range(cols // LANES):
                span = slice(c * LANES, (c + 1) * LANES)
                total = jnp.zeros((dec_len, LANES), F32)
                for ref, s in zip(part_refs, shares):
                    f = jnp.where(left, s[:, 2 * c : 2 * c + 1], s[:, 2 * c + 1 : 2 * c + 2])
                    total = total + ref[j, :, span].astype(F32) * f
                rows_ref[j * dec_len : (j + 1) * dec_len, span] = total.astype(BF16)

    out_ref[0] = jnp.dot(rows_ref[...], w_ref[...], preferred_element_type=F32).astype(BF16)


def project(order, partials, weight):
    parts = len(partials)
    per, dec_len, wide = partials[0].shape
    cols = wide - LANES
    heads = cols // HD
    count = order.shape[0]
    piece = weight.shape[1] // count
    rows = per * dec_len
    return pl.pallas_call(
        functools.partial(project_kernel, heads, parts),
        grid_spec=pltpu.PrefetchScalarGridSpec(
            num_scalar_prefetch=1,
            grid=(count,),
            in_specs=[pl.BlockSpec((per, dec_len, wide), lambda i, o: (0, 0, 0))] * parts
            + [pl.BlockSpec((cols, piece), lambda i, o: (0, o[i]))],
            out_specs=pl.BlockSpec((1, rows, piece), lambda i, o: (i, 0, 0)),
            scratch_shapes=[pltpu.VMEM((rows, cols), BF16)],
        ),
        out_shape=jax.ShapeDtypeStruct((count, rows, piece), BF16),
        cost_estimate=cost(2 * rows * cols * weight.shape[1], cols * weight.shape[1] * 2),
        name="project",
    )(order, *partials, weight)


def body(
    states, enc_gain, dec_states, dec_gain, query_weight, key_value_weight, out_weight, question_of
):
    width = states.shape[-1]
    plen = states.shape[2]
    n_set = lax.axis_size("qset")
    n_seq = lax.axis_size("seq")
    me_set = lax.axis_index("qset")
    me_seq = lax.axis_index("seq")
    per, dec_len = dec_states.shape[0], dec_states.shape[1]
    chips = n_seq // 2
    chip, core = me_seq // 2, me_seq % 2
    piece = width // CHUNKS

    def seq_move(hop, flip):
        return [(s, 2 * ((s // 2 + hop) % chips) + ((s % 2) ^ flip)) for s in range(n_seq)]

    def set_move(hop):
        return [(s, (s + hop) % n_set) for s in range(n_set)]

    own = enc_norm(states[0, 0], enc_gain.reshape(1, width))
    arrived = []
    for c in range(CHUNKS):
        held = []
        for hop in range(chips):
            here = own[c] if hop == 0 else lax.ppermute(own[c], "seq", seq_move(hop, 0))
            held += [here, lax.ppermute(here, "seq", seq_move(0, 1))]
        arrived.append(held)
    slot_seq = jnp.stack(
        [2 * ((chip - hop) % chips) + (core ^ f) for hop in range(chips) for f in range(2)]
    )

    queries = query_rows(
        dec_states.reshape(per * dec_len, width), dec_gain.reshape(1, width), query_weight
    )
    all_queries = [queries] + [
        lax.ppermute(queries, "qset", set_move(hop)) for hop in range(1, n_set)
    ]

    passages = lax.dynamic_index_in_dim(question_of[:, :, 0], me_set, 0, keepdims=False)
    passages = passages[slot_seq]
    owner, number = passages // per, passages % per
    query_slot = ((me_set - owner) % n_set) * per + number
    out_slot = ((owner - me_set) % n_set) * per + number
    index = jnp.arange(n_seq, dtype=jnp.int32)
    named = out_slot[None, :] == jnp.arange(n_set * per, dtype=jnp.int32)[:, None]
    high = jnp.max(jnp.where(named, index[None, :], -1), axis=1)
    low = jnp.min(jnp.where(named, index[None, :], n_seq), axis=1)
    first = jnp.where(high >= 0, low, -1)
    second = jnp.where(high > low, high, -1)
    size = max(n_seq, n_set * per)
    table = jnp.stack([jnp.pad(v, (0, size - v.shape[0])) for v in (query_slot, first, second)])

    acc = None
    for c in range(CHUNKS):
        rows = jnp.concatenate(arrived[c], axis=0)
        part = jnp.einsum(
            "rd,dkc->rkc",
            rows,
            key_value_weight[c * piece : (c + 1) * piece],
            preferred_element_type=F32,
        )
        acc = part if acc is None else acc + part
    kv = jnp.transpose(acc.astype(BF16), (1, 0, 2))

    sent = attend(table, all_queries, kv, n_seq, plen, per, dec_len)
    partials = [sent[0]] + [
        lax.ppermute(sent[hop], "qset", set_move(hop)) for hop in range(1, n_set)
    ]

    moves = [(hop, f) for hop in range(chips) for f in range(2)]
    order = jnp.stack([2 * ((chip + hop) % chips) + (core ^ f) for hop, f in moves])
    out = project(order.astype(jnp.int32), partials, out_weight)
    total = out[0].astype(F32)
    for i, (hop, f) in enumerate(moves):
        if i:
            total = total + lax.ppermute(out[i], "seq", seq_move(hop, f)).astype(F32)
    cols = width // n_seq
    residual = lax.dynamic_slice_in_dim(dec_states, me_seq * cols, cols, 2).astype(F32)
    return (residual + total.reshape(per, dec_len, cols)).astype(BF16)


def solution(mesh):
    return jax.shard_map(
        body,
        mesh=mesh,
        in_specs=(
            P(("groups", "qset"), "seq", None, None),
            P(),
            P(("groups", "qset"), None, None),
            P(),
            P(None, "seq"),
            P(None, None, "seq"),
            P("seq", None),
            P("groups", None, None),
        ),
        out_specs=P(("groups", "qset"), None, "seq"),
        check_vma=False,
    )
```

```python
import functools

import jax
import jax.numpy as jnp
from jax import lax
from jax.experimental import pallas as pl
from jax.experimental.pallas import tpu as pltpu
from jax.sharding import PartitionSpec as P


HD = 64
EPSILON = 1e-06
EMPTY = -1e30
LANES = 128
CUTS = (0, 8, 13, 16)


F32 = jnp.float32
BF16 = jnp.bfloat16


def cost(flops, bytes_accessed):
    return pl.CostEstimate(flops=int(flops), bytes_accessed=int(bytes_accessed), transcendentals=0)


def full_spec():
    return pl.BlockSpec(memory_space=pltpu.VMEM)


def enc_norm_kernel(x_ref, g_ref, *out_refs):
    x = x_ref[...].astype(F32)
    scale = lax.rsqrt(jnp.mean(x * x, axis=-1, keepdims=True) + EPSILON)
    gain = g_ref[...].astype(F32)
    block = 0
    for out in out_refs:
        for i in range(out.shape[1] // LANES):
            part = x_ref[:, block * LANES : (block + 1) * LANES].astype(F32)
            out[:, i * LANES : (i + 1) * LANES] = (part * scale * gain[block : block + 1]).astype(BF16)
            block += 1


def enc_norm(x, gain, cuts):
    rows, width = x.shape
    return pl.pallas_call(
        enc_norm_kernel,
        grid=(1,),
        in_specs=[
            pl.BlockSpec((rows, width), lambda i: (0, 0)),
            pl.BlockSpec((width // LANES, LANES), lambda i: (0, 0)),
        ],
        out_specs=[full_spec()] * (len(cuts) - 1),
        out_shape=[jax.ShapeDtypeStruct((rows, b - a), BF16) for a, b in zip(cuts, cuts[1:])],
        cost_estimate=cost(2e10, rows * width * 4),
        compiler_params=pltpu.CompilerParams(vmem_limit_bytes=8 << 20),
        name="enc_norm",
    )(x, gain.reshape(width // LANES, LANES))


def query_kernel(x_hbm, g_ref, w_hbm, out_ref, x_ref, w_ref, rows_ref, sems):
    pieces = sems.shape[0] - 1
    depth = w_ref.shape[0] // pieces
    cuts = [pl.ds(i * depth, depth) for i in range(pieces)]
    copies = [pltpu.make_async_copy(x_hbm, x_ref, sems.at[pieces])] + [
        pltpu.make_async_copy(w_hbm.at[cut], w_ref.at[cut], sems.at[i])
        for i, cut in enumerate(cuts)
    ]
    for copy in copies:
        copy.start()
    copies[0].wait()
    x = x_ref[...].astype(F32)
    scale = lax.rsqrt(jnp.mean(x * x, axis=-1, keepdims=True) + EPSILON)
    gain = g_ref[...].astype(F32)
    for block in range(x_ref.shape[1] // LANES):
        span = slice(block * LANES, (block + 1) * LANES)
        part = x_ref[:, span].astype(F32) * scale * gain[block : block + 1]
        rows_ref[:, span] = part.astype(BF16)
    total = None
    for copy, cut in zip(copies[1:], cuts):
        copy.wait()
        part = jnp.dot(rows_ref[:, cut], w_ref[cut, :], preferred_element_type=F32)
        total = part if total is None else total + part
    out_ref[...] = total.astype(BF16)


def query_rows(x, gain, weight):
    rows, width = x.shape
    cols = weight.shape[1]
    pieces = 8
    return pl.pallas_call(
        query_kernel,
        in_specs=[
            pl.BlockSpec(memory_space=pl.ANY),
            full_spec(),
            pl.BlockSpec(memory_space=pl.ANY),
        ],
        out_specs=full_spec(),
        out_shape=jax.ShapeDtypeStruct((rows, cols), BF16),
        scratch_shapes=[
            pltpu.VMEM((rows, width), BF16),
            pltpu.VMEM((width, cols), BF16),
            pltpu.VMEM((rows, width), BF16),
            pltpu.SemaphoreType.DMA((pieces + 1,)),
        ],
        cost_estimate=cost(3e9, width * cols * 2),
        compiler_params=pltpu.CompilerParams(vmem_limit_bytes=14 << 20),
        name="query_rows",
    )(x, gain.reshape(width // LANES, LANES), weight)


def sum_kernel(index, res_ref, *refs):
    out_ref = refs[-1]
    per = out_ref.shape[0]
    count = len(refs[:-1]) // per
    for j in range(per):
        total = res_ref[j].astype(F32)
        for ref in refs[j * count : (j + 1) * count]:
            total = total + ref[...].astype(F32)
        out_ref[j] = total.astype(BF16)


def sum_parts(index, residual, parts):
    per, dec_len, _ = residual.shape
    cols = parts[0].shape[1]
    return pl.pallas_call(
        sum_kernel,
        grid_spec=pltpu.PrefetchScalarGridSpec(
            num_scalar_prefetch=1,
            grid=(1,),
            in_specs=[pl.BlockSpec((per, dec_len, cols), lambda i, s: (0, 0, s[0]))]
            + [full_spec()] * len(parts),
            out_specs=pl.BlockSpec((per, dec_len, cols), lambda i, s: (0, 0, 0)),
        ),
        out_shape=jax.ShapeDtypeStruct((per, dec_len, cols), BF16),
        cost_estimate=cost(per * dec_len * cols * 8, per * dec_len * cols * 12),
        compiler_params=pltpu.CompilerParams(vmem_limit_bytes=8 << 20),
        name="sum_parts",
    )(index, residual, *parts)


def load_kernel(cuts, step, src, *refs):
    dests, sems = refs[:-1], refs[-1]
    copies = []
    for a, b, dest in zip(cuts, cuts[1:], dests):
        for low in range(a, b, step):
            size = min(step, b - low)
            copies.append(
                pltpu.make_async_copy(
                    src.at[pl.ds(low, size)], dest.at[pl.ds(low - a, size)], sems.at[len(copies)]
                )
            )
    for copy in copies:
        copy.start()
    for copy in copies:
        copy.wait()


def load(array, cuts, step, limit):
    shapes = [(b - a,) + array.shape[1:] for a, b in zip(cuts, cuts[1:])]
    count = sum(-(-(b - a) // step) for a, b in zip(cuts, cuts[1:]))
    return pl.pallas_call(
        functools.partial(load_kernel, cuts, step),
        in_specs=[pl.BlockSpec(memory_space=pl.ANY)],
        out_specs=[full_spec()] * len(shapes),
        out_shape=[jax.ShapeDtypeStruct(s, BF16) for s in shapes],
        scratch_shapes=[pltpu.SemaphoreType.DMA((count,))],
        cost_estimate=cost(7e9, 2 * array.size),
        compiler_params=pltpu.CompilerParams(vmem_limit_bytes=limit),
    )(array)


def split3(x):
    hi = x.astype(BF16)
    rest = x - hi.astype(F32)
    mid = rest.astype(BF16)
    low = (rest - mid.astype(F32)).astype(BF16)
    return hi, mid, low


def attend_kernel(n_pass, plen, heads, dests, table, *refs):
    q_refs = refs[:dests]
    kv_ref = refs[dests]
    out_refs = refs[dests + 1 : -7]
    qs, score_s, weight_s, part, peak_s, total_s, stat_s = refs[-7:]
    dec_len, cols = out_refs[0].shape[0], heads * HD
    per = len(out_refs) // dests
    wide = score_s.shape[1] // dec_len
    span_w = wide * HD
    groups = cols // span_w
    for i, ref in enumerate(q_refs):
        for j in range(per):
            qs[i * per + j] = ref[j * dec_len : (j + 1) * dec_len, :]
    head_of = lax.broadcasted_iota(jnp.int32, (dec_len, span_w), 1) // HD
    lane = lax.broadcasted_iota(jnp.int32, (dec_len, LANES), 1)
    units = [(p, g) for p in range(n_pass) for g in range(groups)]

    def pick(stacked):
        kept = stacked[:dec_len]
        for h in range(1, wide):
            kept = jnp.where(head_of == h, stacked[h * dec_len : (h + 1) * dec_len], kept)
        return kept

    for p, g in units:
        span = slice(g * span_w, (g + 1) * span_w)
        q = qs[table[0, p], :, span]
        zero = jnp.zeros_like(q)
        stacked = jnp.concatenate([jnp.where(head_of == h, q, zero) for h in range(wide)], axis=0)
        score_s[p * groups + g] = lax.dot_general(
            stacked,
            kv_ref[0, p * plen : (p + 1) * plen, span],
            (((1,), (1,)), ((), ())),
            preferred_element_type=F32,
        )
    for p in range(n_pass):
        peaks = jnp.zeros((dec_len, LANES), F32)
        totals = jnp.zeros((dec_len, LANES), F32)
        for g in range(groups):
            u = p * groups + g
            scores = score_s[u]
            peak = jnp.max(scores, axis=-1, keepdims=True)
            weights = jnp.exp(scores - peak)
            total = jnp.sum(weights, axis=-1, keepdims=True)
            weight_s[u] = weights.astype(BF16)
            span = slice(g * span_w, (g + 1) * span_w)
            peak_s[p, :, span] = pick(jnp.broadcast_to(peak, (peak.shape[0], span_w)))
            total_s[p, :, span] = pick(jnp.broadcast_to(total, (total.shape[0], span_w)))
            for h in range(wide):
                here = lane == g * wide + h
                rows = slice(h * dec_len, (h + 1) * dec_len)
                peaks = jnp.where(here, peak[rows], peaks)
                totals = jnp.where(here, total[rows], totals)
        stat_s[p, 0] = peaks
        stat_s[p, 1] = totals
    for p, g in units:
        span = slice(g * span_w, (g + 1) * span_w)
        summed = jnp.dot(
            weight_s[p * groups + g],
            kv_ref[1, p * plen : (p + 1) * plen, span],
            preferred_element_type=F32,
        )
        part[p, :, span] = pick(summed)

    def put_stats(out, peaks, totals):
        p_hi, p_mid, p_low = split3(peaks)
        t_hi, t_low, _ = split3(totals)
        packed = jnp.concatenate(
            [v[:, :heads] for v in (p_hi, p_mid, p_low, t_hi, t_low)]
            + [jnp.zeros((dec_len, LANES - 5 * heads), BF16)],
            axis=1,
        )
        out[:, cols:] = packed

    for t, out in enumerate(out_refs):
        a, b = table[1, t], table[2, t]

        @pl.when(a < 0)
        def _():
            out[:, :cols] = jnp.zeros((dec_len, cols), BF16)
            put_stats(out, jnp.full((dec_len, LANES), EMPTY, F32), jnp.zeros((dec_len, LANES), F32))

        @pl.when((a >= 0) & (b < 0))
        def _():
            out[:, :cols] = (part[a] / total_s[a]).astype(BF16)
            put_stats(out, stat_s[a, 0], stat_s[a, 1])

        @pl.when((a >= 0) & (b >= 0))
        def _():
            top = jnp.maximum(peak_s[a], peak_s[b])
            f_a, f_b = jnp.exp(peak_s[a] - top), jnp.exp(peak_s[b] - top)
            whole = total_s[a] * f_a + total_s[b] * f_b
            out[:, :cols] = ((part[a] * f_a + part[b] * f_b) / whole).astype(BF16)
            peaks = jnp.maximum(stat_s[a, 0], stat_s[b, 0])
            totals = stat_s[a, 1] * jnp.exp(stat_s[a, 0] - peaks) + stat_s[b, 1] * jnp.exp(
                stat_s[b, 0] - peaks
            )
            put_stats(out, peaks, totals)


def attend(table, queries, kv, n_pass, plen, per, dec_len):
    dests = len(queries)
    cols = queries[0].shape[1]
    heads = cols // HD
    rows = n_pass * dec_len
    wide = min(heads, 4)
    units = n_pass * heads // wide
    return pl.pallas_call(
        functools.partial(attend_kernel, n_pass, plen, heads, dests),
        in_specs=[pl.BlockSpec(memory_space=pltpu.SMEM)] + [full_spec()] * (dests + 1),
        out_specs=[full_spec()] * (dests * per),
        out_shape=[jax.ShapeDtypeStruct((dec_len, cols + LANES), BF16)] * (dests * per),
        scratch_shapes=[
            pltpu.VMEM((dests * per, dec_len, cols), BF16),
            pltpu.VMEM((units, wide * dec_len, plen), F32),
            pltpu.VMEM((units, wide * dec_len, plen), BF16),
            pltpu.VMEM((n_pass, dec_len, cols), F32),
            pltpu.VMEM((n_pass, dec_len, cols), F32),
            pltpu.VMEM((n_pass, dec_len, cols), F32),
            pltpu.VMEM((n_pass, 2, dec_len, LANES), F32),
        ],
        cost_estimate=cost(8 * rows * plen * cols, n_pass * plen * cols * 4),
        compiler_params=pltpu.CompilerParams(vmem_limit_bytes=20 << 20),
        name="attend",
    )(table, *queries, kv)


def project_kernel(heads, parts, order, *refs):
    part_refs = refs[:parts]
    w_ref = refs[parts]
    out_refs = refs[parts + 1 : -1]
    rows_ref = refs[-1]
    dec_len, cols = part_refs[0].shape[0], heads * HD
    row = lax.broadcasted_iota(jnp.int32, (LANES, cols), 0)
    head = lax.broadcasted_iota(jnp.int32, (LANES, cols), 1) // HD
    same = (row % heads == head).astype(F32)
    spread_peak = jnp.where(row < 3 * heads, same, 0.0).astype(BF16)
    spread_total = jnp.where((row >= 3 * heads) & (row < 5 * heads), same, 0.0).astype(BF16)
    stats = jnp.concatenate([ref[:, cols:] for ref in part_refs], axis=0)
    peaks = jnp.dot(stats, spread_peak, preferred_element_type=F32)
    totals = jnp.dot(stats, spread_total, preferred_element_type=F32)
    peaks = [peaks[i * dec_len : (i + 1) * dec_len] for i in range(parts)]
    totals = [totals[i * dec_len : (i + 1) * dec_len] for i in range(parts)]
    top = functools.reduce(jnp.maximum, peaks)
    sizes = [t * jnp.exp(p - top) for p, t in zip(peaks, totals)]
    mixed = functools.reduce(
        jnp.add, [ref[:, :cols].astype(F32) * s for ref, s in zip(part_refs, sizes)]
    )
    rows_ref[...] = (mixed / functools.reduce(jnp.add, sizes)).astype(BF16)
    piece = out_refs[0].shape[1]
    for i, out in enumerate(out_refs):
        cut = pl.ds(pl.multiple_of(order[i] * piece, piece), piece)
        out[...] = jnp.dot(rows_ref[...], w_ref[:, cut], preferred_element_type=F32).astype(BF16)


def project(order, partials, weight):
    parts = len(partials)
    rows, wide = partials[0].shape
    cols = wide - LANES
    heads = cols // HD
    count = order.shape[0]
    piece = weight.shape[1] // count
    return pl.pallas_call(
        functools.partial(project_kernel, heads, parts),
        in_specs=[pl.BlockSpec(memory_space=pltpu.SMEM)] + [full_spec()] * (parts + 1),
        out_specs=[full_spec()] * count,
        out_shape=[jax.ShapeDtypeStruct((rows, piece), BF16)] * count,
        scratch_shapes=[pltpu.VMEM((rows, cols), BF16)],
        cost_estimate=cost(2 * rows * cols * weight.shape[1], cols * weight.shape[1] * 2),
        compiler_params=pltpu.CompilerParams(vmem_limit_bytes=16 << 20),
        name="project",
    )(order, *partials, weight)


def body(
    states, enc_gain, dec_states, dec_gain, query_weight, key_value_weight, out_weight, question_of
):
    width = states.shape[-1]
    plen = states.shape[2]
    n_set = lax.axis_size("qset")
    n_seq = lax.axis_size("seq")
    me_set = lax.axis_index("qset")
    me_seq = lax.axis_index("seq")
    per, dec_len = dec_states.shape[0], dec_states.shape[1]
    chips = n_seq // 2
    chip, core = me_seq // 2, me_seq % 2
    cuts = [width * c // 16 for c in CUTS]

    def seq_move(hop, flip):
        return [(s, 2 * ((s // 2 + hop) % chips) + ((s % 2) ^ flip)) for s in range(n_seq)]

    def set_move(hop):
        return [(s, (s + hop) % n_set) for s in range(n_set)]

    def cross(own):
        return [lax.ppermute(own, "seq", seq_move(hop, 0)) for hop in range(1, chips)]

    def sibling(rows):
        return lax.ppermute(rows, "seq", seq_move(0, 1))

    own = list(enc_norm(states[0, 0], enc_gain, cuts))
    queries = query_rows(dec_states.reshape(per * dec_len, width), dec_gain, query_weight)
    crossed = [cross(rows) for rows in own]
    slot_seq = jnp.stack(
        [2 * ((chip - hop) % chips) + (core ^ f) for hop in range(chips) for f in range(2)]
    )

    all_queries = [queries] + [
        lax.ppermute(queries, "qset", set_move(hop)) for hop in range(1, n_set)
    ]

    passages = lax.dynamic_index_in_dim(question_of[:, :, 0], me_set, 0, keepdims=False)
    passages = passages[slot_seq]
    owner, number = passages // per, passages % per
    query_slot = ((me_set - owner) % n_set) * per + number
    out_slot = ((owner - me_set) % n_set) * per + number
    index = jnp.arange(n_seq, dtype=jnp.int32)
    named = out_slot[None, :] == jnp.arange(n_set * per, dtype=jnp.int32)[:, None]
    high = jnp.max(jnp.where(named, index[None, :], -1), axis=1)
    low = jnp.min(jnp.where(named, index[None, :], n_seq), axis=1)
    first = jnp.where(high >= 0, low, -1)
    second = jnp.where(high > low, high, -1)
    size = max(n_seq, n_set * per)
    table = jnp.stack([jnp.pad(v, (0, size - v.shape[0])) for v in (query_slot, first, second)])

    kv_parts = load(key_value_weight, cuts, 4096, 20 << 20)
    acc, forwarded = None, ()
    for c, weight in enumerate(kv_parts):
        beside = sibling(own[c])
        here, _ = lax.optimization_barrier((crossed[c], (forwarded, acc if c > 1 else ())))
        forwarded = [sibling(rows) for rows in here]
        chunks = [own[c], beside]
        for pair in zip(here, forwarded):
            chunks += pair
        part = jnp.einsum(
            "rd,dkc->rkc", jnp.concatenate(chunks, axis=0), weight, preferred_element_type=F32
        )
        acc = part if acc is None else acc + part
    kv = jnp.transpose(acc.astype(BF16), (1, 0, 2))

    sent = list(attend(table, all_queries, kv, n_seq, plen, per, dec_len))
    out_source, sent[0] = lax.optimization_barrier((out_weight, sent[0]))
    (out_part,) = load(out_source, [0, out_weight.shape[0]], 256, 20 << 20)
    moves = [(hop, f) for hop in range(chips) for f in range(2)]
    order = jnp.stack([2 * ((chip + hop) % chips) + (core ^ f) for hop, f in moves])
    order = order.astype(jnp.int32)

    partials = []
    for j in range(per):
        partials.append(
            [sent[j]]
            + [lax.ppermute(sent[hop * per + j], "qset", set_move(hop)) for hop in range(1, n_set)]
        )
    parts = []
    for j in range(per):
        out = project(order, partials[j], out_part)
        parts += [out[0]] + [
            lax.ppermute(out[i], "seq", seq_move(*moves[i])) for i in range(1, len(moves))
        ]
    return sum_parts(me_seq.reshape(1).astype(jnp.int32), dec_states, parts)


def solution(mesh):
    return jax.shard_map(
        body,
        mesh=mesh,
        in_specs=(
            P(("groups", "qset"), "seq", None, None),
            P(),
            P(("groups", "qset"), None, None),
            P(),
            P(None, "seq"),
            P(None, None, "seq"),
            P("seq", None),
            P("groups", None, None),
        ),
        out_specs=P(("groups", "qset"), None, "seq"),
        check_vma=False,
    )
```

```python
import functools

import jax
import jax.numpy as jnp
from jax import lax
from jax.experimental import pallas as pl
from jax.experimental.pallas import tpu as pltpu
from jax.sharding import PartitionSpec as P


HD = 64
EPSILON = 1e-06
EMPTY = -1e30
LANES = 128
CUTS = (0, 7, 12, 16)


F32 = jnp.float32
BF16 = jnp.bfloat16


def cost(flops, bytes_accessed):
    return pl.CostEstimate(flops=int(flops), bytes_accessed=int(bytes_accessed), transcendentals=0)


def full_spec():
    return pl.BlockSpec(memory_space=pltpu.VMEM)


def enc_norm_kernel(x_ref, g_ref, *out_refs):
    x = x_ref[...].astype(F32)
    scale = lax.rsqrt(jnp.mean(x * x, axis=-1, keepdims=True) + EPSILON)
    gain = g_ref[...].astype(F32)
    block = 0
    for out in out_refs:
        for i in range(out.shape[1] // LANES):
            part = x_ref[:, block * LANES : (block + 1) * LANES].astype(F32)
            out[:, i * LANES : (i + 1) * LANES] = (part * scale * gain[block : block + 1]).astype(BF16)
            block += 1


def enc_norm(x, gain, cuts):
    rows, width = x.shape
    return pl.pallas_call(
        enc_norm_kernel,
        grid=(1,),
        in_specs=[
            pl.BlockSpec((rows, width), lambda i: (0, 0)),
            pl.BlockSpec((width // LANES, LANES), lambda i: (0, 0)),
        ],
        out_specs=[full_spec()] * (len(cuts) - 1),
        out_shape=[jax.ShapeDtypeStruct((rows, b - a), BF16) for a, b in zip(cuts, cuts[1:])],
        cost_estimate=cost(2e10, rows * width * 4),
        compiler_params=pltpu.CompilerParams(vmem_limit_bytes=8 << 20),
        name="enc_norm",
    )(x, gain.reshape(width // LANES, LANES))


def query_kernel(x_hbm, g_ref, w_hbm, out_ref, x_ref, w_ref, rows_ref, sems):
    pieces = sems.shape[0] - 1
    depth = w_ref.shape[0] // pieces
    cuts = [pl.ds(i * depth, depth) for i in range(pieces)]
    copies = [pltpu.make_async_copy(x_hbm, x_ref, sems.at[pieces])] + [
        pltpu.make_async_copy(w_hbm.at[cut], w_ref.at[cut], sems.at[i])
        for i, cut in enumerate(cuts)
    ]
    for copy in copies:
        copy.start()
    copies[0].wait()
    x = x_ref[...].astype(F32)
    scale = lax.rsqrt(jnp.mean(x * x, axis=-1, keepdims=True) + EPSILON)
    gain = g_ref[...].astype(F32)
    for block in range(x_ref.shape[1] // LANES):
        span = slice(block * LANES, (block + 1) * LANES)
        part = x_ref[:, span].astype(F32) * scale * gain[block : block + 1]
        rows_ref[:, span] = part.astype(BF16)
    total = None
    for copy, cut in zip(copies[1:], cuts):
        copy.wait()
        part = jnp.dot(rows_ref[:, cut], w_ref[cut, :], preferred_element_type=F32)
        total = part if total is None else total + part
    out_ref[...] = total.astype(BF16)


def query_rows(x, gain, weight):
    rows, width = x.shape
    cols = weight.shape[1]
    pieces = 8
    return pl.pallas_call(
        query_kernel,
        in_specs=[
            pl.BlockSpec(memory_space=pl.ANY),
            full_spec(),
            pl.BlockSpec(memory_space=pl.ANY),
        ],
        out_specs=full_spec(),
        out_shape=jax.ShapeDtypeStruct((rows, cols), BF16),
        scratch_shapes=[
            pltpu.VMEM((rows, width), BF16),
            pltpu.VMEM((width, cols), BF16),
            pltpu.VMEM((rows, width), BF16),
            pltpu.SemaphoreType.DMA((pieces + 1,)),
        ],
        cost_estimate=cost(3e9, width * cols * 2),
        compiler_params=pltpu.CompilerParams(vmem_limit_bytes=14 << 20),
        name="query_rows",
    )(x, gain.reshape(width // LANES, LANES), weight)


def sum_kernel(index, res_ref, *refs):
    out_ref = refs[-1]
    per = out_ref.shape[0]
    count = len(refs[:-1]) // per
    for j in range(per):
        total = res_ref[j].astype(F32)
        for ref in refs[j * count : (j + 1) * count]:
            total = total + ref[...].astype(F32)
        out_ref[j] = total.astype(BF16)


def sum_parts(index, residual, parts):
    per, dec_len, _ = residual.shape
    cols = parts[0].shape[1]
    return pl.pallas_call(
        sum_kernel,
        grid_spec=pltpu.PrefetchScalarGridSpec(
            num_scalar_prefetch=1,
            grid=(1,),
            in_specs=[pl.BlockSpec((per, dec_len, cols), lambda i, s: (0, 0, s[0]))]
            + [full_spec()] * len(parts),
            out_specs=pl.BlockSpec((per, dec_len, cols), lambda i, s: (0, 0, 0)),
        ),
        out_shape=jax.ShapeDtypeStruct((per, dec_len, cols), BF16),
        cost_estimate=cost(per * dec_len * cols * 8, per * dec_len * cols * 12),
        compiler_params=pltpu.CompilerParams(vmem_limit_bytes=8 << 20),
        name="sum_parts",
    )(index, residual, *parts)


def load_kernel(cuts, step, src, *refs):
    dests, sems = refs[:-1], refs[-1]
    copies = []
    for a, b, dest in zip(cuts, cuts[1:], dests):
        for low in range(a, b, step):
            size = min(step, b - low)
            copies.append(
                pltpu.make_async_copy(
                    src.at[pl.ds(low, size)], dest.at[pl.ds(low - a, size)], sems.at[len(copies)]
                )
            )
    for copy in copies:
        copy.start()
    for copy in copies:
        copy.wait()


def load(array, cuts, step, limit):
    shapes = [(b - a,) + array.shape[1:] for a, b in zip(cuts, cuts[1:])]
    count = sum(-(-(b - a) // step) for a, b in zip(cuts, cuts[1:]))
    return pl.pallas_call(
        functools.partial(load_kernel, cuts, step),
        in_specs=[pl.BlockSpec(memory_space=pl.ANY)],
        out_specs=[full_spec()] * len(shapes),
        out_shape=[jax.ShapeDtypeStruct(s, BF16) for s in shapes],
        scratch_shapes=[pltpu.SemaphoreType.DMA((count,))],
        cost_estimate=cost(7e9, 2 * array.size),
        compiler_params=pltpu.CompilerParams(vmem_limit_bytes=limit),
    )(array)


def split3(x):
    hi = x.astype(BF16)
    rest = x - hi.astype(F32)
    mid = rest.astype(BF16)
    low = (rest - mid.astype(F32)).astype(BF16)
    return hi, mid, low


def fill_table(question_ref, table, n_pass, per, n_set):
    chips = n_pass // 2
    me_set, me_seq = lax.axis_index("qset"), lax.axis_index("seq")
    chip = lax.div(me_seq, 2)
    core = me_seq - 2 * chip
    for t in range(n_set * per):
        table[1, t] = -1
        table[2, t] = -1
    for i in range(n_pass):
        hop, flip = divmod(i, 2)
        source = 2 * lax.rem(chip + chips - hop, chips) + (1 - core if flip else core)
        question = question_ref[me_set, source]
        owner = lax.div(question, per)
        number = question - owner * per
        table[0, i] = lax.rem(me_set + n_set - owner, n_set) * per + number
        t = lax.rem(owner + n_set - me_set, n_set) * per + number
        row = jnp.where(table[1, t] < 0, 1, 2)
        table[row, t] = i


def attend_kernel(n_pass, plen, heads, dests, question_ref, *refs):
    q_refs = refs[:dests]
    kv_ref = refs[dests]
    out_refs = refs[dests + 1 : -9]
    qs, score_s, weight_s, part, peak_s, total_s, stat_s, sent_s, table = refs[-9:]
    dec_len, cols = out_refs[0].shape[0], heads * HD
    per = len(out_refs) // dests
    fill_table(question_ref, table, n_pass, per, dests)
    wide = score_s.shape[1] // dec_len
    span_w = wide * HD
    groups = cols // span_w
    for i, ref in enumerate(q_refs):
        for j in range(per):
            qs[i * per + j] = ref[j * dec_len : (j + 1) * dec_len, :]
    head_of = lax.broadcasted_iota(jnp.int32, (dec_len, span_w), 1) // HD
    lane = lax.broadcasted_iota(jnp.int32, (dec_len, LANES), 1)
    units = [(p, g) for p in range(n_pass) for g in range(groups)]

    def pick(stacked):
        kept = stacked[:dec_len]
        for h in range(1, wide):
            kept = jnp.where(head_of == h, stacked[h * dec_len : (h + 1) * dec_len], kept)
        return kept

    for p, g in units:
        span = slice(g * span_w, (g + 1) * span_w)
        q = qs[table[0, p], :, span]
        zero = jnp.zeros_like(q)
        stacked = jnp.concatenate([jnp.where(head_of == h, q, zero) for h in range(wide)], axis=0)
        score_s[p * groups + g] = lax.dot_general(
            stacked,
            kv_ref[0, p * plen : (p + 1) * plen, span],
            (((1,), (1,)), ((), ())),
            preferred_element_type=F32,
        )
    for p in range(n_pass):
        peaks = jnp.zeros((dec_len, LANES), F32)
        totals = jnp.zeros((dec_len, LANES), F32)
        for g in range(groups):
            u = p * groups + g
            scores = score_s[u]
            peak = jnp.max(scores, axis=-1, keepdims=True)
            weights = jnp.exp(scores - peak)
            total = jnp.sum(weights, axis=-1, keepdims=True)
            weight_s[u] = weights.astype(BF16)
            span = slice(g * span_w, (g + 1) * span_w)
            peak_s[p, :, span] = pick(jnp.broadcast_to(peak, (peak.shape[0], span_w)))
            total_s[p, :, span] = pick(jnp.broadcast_to(total, (total.shape[0], span_w)))
            for h in range(wide):
                here = lane == g * wide + h
                rows = slice(h * dec_len, (h + 1) * dec_len)
                peaks = jnp.where(here, peak[rows], peaks)
                totals = jnp.where(here, total[rows], totals)
        stat_s[p, 0] = peaks
        stat_s[p, 1] = totals
    for p, g in units:
        span = slice(g * span_w, (g + 1) * span_w)
        summed = jnp.dot(
            weight_s[p * groups + g],
            kv_ref[1, p * plen : (p + 1) * plen, span],
            preferred_element_type=F32,
        )
        part[p, :, span] = pick(summed)

    for t, out in enumerate(out_refs):
        a, b = table[1, t], table[2, t]

        @pl.when(a < 0)
        def _():
            out[:, :cols] = jnp.zeros((dec_len, cols), BF16)
            sent_s[t, 0] = jnp.full((dec_len, LANES), EMPTY, F32)
            sent_s[t, 1] = jnp.zeros((dec_len, LANES), F32)

        @pl.when((a >= 0) & (b < 0))
        def _():
            out[:, :cols] = (part[a] / total_s[a]).astype(BF16)
            sent_s[t] = stat_s[a]

        @pl.when((a >= 0) & (b >= 0))
        def _():
            top = jnp.maximum(peak_s[a], peak_s[b])
            f_a, f_b = jnp.exp(peak_s[a] - top), jnp.exp(peak_s[b] - top)
            whole = total_s[a] * f_a + total_s[b] * f_b
            out[:, :cols] = ((part[a] * f_a + part[b] * f_b) / whole).astype(BF16)
            peaks = jnp.maximum(stat_s[a, 0], stat_s[b, 0])
            sent_s[t, 0] = peaks
            sent_s[t, 1] = stat_s[a, 1] * jnp.exp(stat_s[a, 0] - peaks) + stat_s[b, 1] * jnp.exp(
                stat_s[b, 0] - peaks
            )

    for r in range(dests):
        pieces = []
        for t in range(r * per, (r + 1) * per):
            for piece in (*split3(sent_s[t, 0]), sent_s[t, 1].astype(BF16)):
                pieces.append(piece[:, :heads])
        room = out_refs[r * per].shape[1] - cols - 4 * heads * per
        if room:
            pieces.append(jnp.zeros((dec_len, room), BF16))
        out_refs[r * per][:, cols:] = jnp.concatenate(pieces, axis=1)


def attend(questions, queries, kv, n_pass, plen, per, dec_len):
    dests = len(queries)
    cols = queries[0].shape[1]
    heads = cols // HD
    rows = n_pass * dec_len
    wide = min(heads, 4)
    units = n_pass * heads // wide
    extra = -(-4 * heads * per // LANES) * LANES
    return pl.pallas_call(
        functools.partial(attend_kernel, n_pass, plen, heads, dests),
        in_specs=[pl.BlockSpec(memory_space=pltpu.SMEM)] + [full_spec()] * (dests + 1),
        out_specs=[full_spec()] * (dests * per),
        out_shape=[
            jax.ShapeDtypeStruct((dec_len, cols if t % per else cols + extra), BF16)
            for t in range(dests * per)
        ],
        scratch_shapes=[
            pltpu.VMEM((dests * per, dec_len, cols), BF16),
            pltpu.VMEM((units, wide * dec_len, plen), F32),
            pltpu.VMEM((units, wide * dec_len, plen), BF16),
            pltpu.VMEM((n_pass, dec_len, cols), F32),
            pltpu.VMEM((n_pass, dec_len, cols), F32),
            pltpu.VMEM((n_pass, dec_len, cols), F32),
            pltpu.VMEM((n_pass, 2, dec_len, LANES), F32),
            pltpu.VMEM((dests * per, 2, dec_len, LANES), F32),
            pltpu.SMEM((3, max(n_pass, dests * per)), jnp.int32),
        ],
        cost_estimate=cost(8 * rows * plen * cols, n_pass * plen * cols * 4),
        compiler_params=pltpu.CompilerParams(vmem_limit_bytes=20 << 20),
        name="attend",
    )(questions, *queries, kv)


def project_kernel(heads, parts, number, *refs):
    part_refs, stat_refs = refs[:parts], refs[parts : 2 * parts]
    w_ref = refs[2 * parts]
    out_refs, rows_ref = refs[2 * parts + 1 : -1], refs[-1]
    dec_len, cols = part_refs[0].shape[0], heads * HD
    stats = jnp.concatenate([ref[:, cols:] for ref in stat_refs], axis=0)
    row = lax.broadcasted_iota(jnp.int32, (stats.shape[1], cols), 0) - number * 4 * heads
    head = lax.broadcasted_iota(jnp.int32, (stats.shape[1], cols), 1) // HD
    is_peak = functools.reduce(jnp.logical_or, [row == head + i * heads for i in range(3)])
    spread_peak = is_peak.astype(F32).astype(BF16)
    spread_total = (row == head + 3 * heads).astype(F32).astype(BF16)
    peaks = jnp.dot(stats, spread_peak, preferred_element_type=F32)
    totals = jnp.dot(stats, spread_total, preferred_element_type=F32)
    peaks = [peaks[i * dec_len : (i + 1) * dec_len] for i in range(parts)]
    totals = [totals[i * dec_len : (i + 1) * dec_len] for i in range(parts)]
    top = functools.reduce(jnp.maximum, peaks)
    sizes = [t * jnp.exp(p - top) for p, t in zip(peaks, totals)]
    mixed = functools.reduce(
        jnp.add, [ref[:, :cols].astype(F32) * s for ref, s in zip(part_refs, sizes)]
    )
    rows_ref[...] = (mixed / functools.reduce(jnp.add, sizes)).astype(BF16)
    piece = out_refs[0].shape[1]
    chips = len(out_refs) // 2
    me_seq = lax.axis_index("seq")
    chip = lax.div(me_seq, 2)
    core = me_seq - 2 * chip
    for i, out in enumerate(out_refs):
        hop, flip = divmod(i, 2)
        dest = 2 * lax.rem(chip + hop, chips) + (1 - core if flip else core)
        cut = pl.ds(pl.multiple_of(dest * piece, piece), piece)
        out[...] = jnp.dot(rows_ref[...], w_ref[:, cut], preferred_element_type=F32).astype(BF16)


def project(number, partials, stats, weight, count):
    parts = len(partials)
    rows = partials[0].shape[0]
    cols = weight.shape[0]
    piece = weight.shape[1] // count
    return pl.pallas_call(
        functools.partial(project_kernel, cols // HD, parts, number),
        in_specs=[full_spec()] * (2 * parts + 1),
        out_specs=[full_spec()] * count,
        out_shape=[jax.ShapeDtypeStruct((rows, piece), BF16)] * count,
        scratch_shapes=[pltpu.VMEM((rows, cols), BF16)],
        cost_estimate=cost(2 * rows * cols * weight.shape[1], cols * weight.shape[1] * 2),
        compiler_params=pltpu.CompilerParams(vmem_limit_bytes=16 << 20),
        name="project",
    )(*partials, *stats, weight)


def body(
    states, enc_gain, dec_states, dec_gain, query_weight, key_value_weight, out_weight, question_of
):
    width = states.shape[-1]
    plen = states.shape[2]
    n_set = lax.axis_size("qset")
    n_seq = lax.axis_size("seq")
    me_seq = lax.axis_index("seq")
    per, dec_len = dec_states.shape[0], dec_states.shape[1]
    chips = n_seq // 2
    cuts = [width * c // 16 for c in CUTS]

    def seq_move(hop, flip):
        return [(s, 2 * ((s // 2 + hop) % chips) + ((s % 2) ^ flip)) for s in range(n_seq)]

    def set_move(hop):
        return [(s, (s + hop) % n_set) for s in range(n_set)]

    def cross(own):
        return [lax.ppermute(own, "seq", seq_move(hop, 0)) for hop in range(1, chips)]

    def sibling(rows):
        return lax.ppermute(rows, "seq", seq_move(0, 1))

    own = list(enc_norm(states[0, 0], enc_gain, cuts))
    queries = query_rows(dec_states.reshape(per * dec_len, width), dec_gain, query_weight)
    crossed = [cross(rows) for rows in own]
    all_queries = [queries] + [
        lax.ppermute(queries, "qset", set_move(hop)) for hop in range(1, n_set)
    ]

    kv_parts = load(key_value_weight, cuts, 256, 28 << 20)
    acc = None
    for c, weight in enumerate(kv_parts):
        beside, here = sibling(own[c]), crossed[c]
        forwarded = [sibling(rows) for rows in here]
        chunks = [own[c], beside]
        for pair in zip(here, forwarded):
            chunks += pair
        part = jnp.einsum(
            "rd,dkc->rkc", jnp.concatenate(chunks, axis=0), weight, preferred_element_type=F32
        )
        acc = part if acc is None else acc + part
    kv = jnp.transpose(acc.astype(BF16), (1, 0, 2))

    sent = list(attend(question_of[:, :, 0], all_queries, kv, n_seq, plen, per, dec_len))
    out_source, sent[0] = lax.optimization_barrier((out_weight, sent[0]))
    (out_part,) = load(out_source, [0, out_weight.shape[0]], 256, 42 << 20)
    moves = [(hop, f) for hop in range(chips) for f in range(2)]

    partials = []
    for j in range(per):
        partials.append(
            [sent[j]]
            + [lax.ppermute(sent[hop * per + j], "qset", set_move(hop)) for hop in range(1, n_set)]
        )
    parts = []
    for j in range(per):
        out = project(j, partials[j], partials[0], out_part, n_seq)
        parts += [out[0]] + [
            lax.ppermute(out[i], "seq", seq_move(*moves[i])) for i in range(1, len(moves))
        ]
    return sum_parts(me_seq.reshape(1).astype(jnp.int32), dec_states, parts)


def solution(mesh):
    return jax.shard_map(
        body,
        mesh=mesh,
        in_specs=(
            P(("groups", "qset"), "seq", None, None),
            P(),
            P(("groups", "qset"), None, None),
            P(),
            P(None, "seq"),
            P(None, None, "seq"),
            P("seq", None),
            P("groups", None, None),
        ),
        out_specs=P(("groups", "qset"), None, "seq"),
        check_vma=False,
    )
```

```python
import functools

import jax
import jax.numpy as jnp
from jax import lax
from jax.experimental import pallas as pl
from jax.experimental.pallas import tpu as pltpu
from jax.sharding import PartitionSpec as P


HD = 64
EPSILON = 1e-06
EMPTY = -1e30
LANES = 128
CUTS = (0, 7, 12, 16)


F32 = jnp.float32
BF16 = jnp.bfloat16


def cost(flops, bytes_accessed):
    return pl.CostEstimate(flops=int(flops), bytes_accessed=int(bytes_accessed), transcendentals=0)


def full_spec():
    return pl.BlockSpec(memory_space=pltpu.VMEM)


def enc_norm_kernel(x_ref, g_ref, *out_refs):
    x = x_ref[...].astype(F32)
    scale = lax.rsqrt(jnp.mean(x * x, axis=-1, keepdims=True) + EPSILON)
    gain = g_ref[...].astype(F32)
    block = 0
    for out in out_refs:
        for i in range(out.shape[1] // LANES):
            part = x_ref[:, block * LANES : (block + 1) * LANES].astype(F32)
            out[:, i * LANES : (i + 1) * LANES] = (part * scale * gain[block : block + 1]).astype(BF16)
            block += 1


def enc_norm(x, gain, cuts):
    rows, width = x.shape
    return pl.pallas_call(
        enc_norm_kernel,
        grid=(1,),
        in_specs=[
            pl.BlockSpec((rows, width), lambda i: (0, 0)),
            pl.BlockSpec((width // LANES, LANES), lambda i: (0, 0)),
        ],
        out_specs=[full_spec()] * (len(cuts) - 1),
        out_shape=[jax.ShapeDtypeStruct((rows, b - a), BF16) for a, b in zip(cuts, cuts[1:])],
        cost_estimate=cost(2e10, rows * width * 4),
        compiler_params=pltpu.CompilerParams(vmem_limit_bytes=8 << 20),
        name="enc_norm",
    )(x, gain.reshape(width // LANES, LANES))


def query_kernel(x_hbm, g_ref, w_hbm, out_ref, x_ref, w_ref, rows_ref, sems):
    pieces = sems.shape[0] - 1
    depth = w_ref.shape[0] // pieces
    cuts = [pl.ds(i * depth, depth) for i in range(pieces)]
    copies = [pltpu.make_async_copy(x_hbm, x_ref, sems.at[pieces])] + [
        pltpu.make_async_copy(w_hbm.at[cut], w_ref.at[cut], sems.at[i])
        for i, cut in enumerate(cuts)
    ]
    for copy in copies:
        copy.start()
    copies[0].wait()
    x = x_ref[...].astype(F32)
    scale = lax.rsqrt(jnp.mean(x * x, axis=-1, keepdims=True) + EPSILON)
    gain = g_ref[...].astype(F32)
    for block in range(x_ref.shape[1] // LANES):
        span = slice(block * LANES, (block + 1) * LANES)
        part = x_ref[:, span].astype(F32) * scale * gain[block : block + 1]
        rows_ref[:, span] = part.astype(BF16)
    total = None
    for copy, cut in zip(copies[1:], cuts):
        copy.wait()
        part = jnp.dot(rows_ref[:, cut], w_ref[cut, :], preferred_element_type=F32)
        total = part if total is None else total + part
    out_ref[...] = total.astype(BF16)


def query_rows(x, gain, weight):
    rows, width = x.shape
    cols = weight.shape[1]
    pieces = 8
    return pl.pallas_call(
        query_kernel,
        in_specs=[
            pl.BlockSpec(memory_space=pl.ANY),
            full_spec(),
            pl.BlockSpec(memory_space=pl.ANY),
        ],
        out_specs=full_spec(),
        out_shape=jax.ShapeDtypeStruct((rows, cols), BF16),
        scratch_shapes=[
            pltpu.VMEM((rows, width), BF16),
            pltpu.VMEM((width, cols), BF16),
            pltpu.VMEM((rows, width), BF16),
            pltpu.SemaphoreType.DMA((pieces + 1,)),
        ],
        cost_estimate=cost(3e9, width * cols * 2),
        compiler_params=pltpu.CompilerParams(vmem_limit_bytes=14 << 20),
        name="query_rows",
    )(x, gain.reshape(width // LANES, LANES), weight)


def sum_kernel(index, res_ref, *refs):
    out_ref = refs[-1]
    per = out_ref.shape[0]
    count = len(refs[:-1]) // per
    for j in range(per):
        total = res_ref[j].astype(F32)
        for ref in refs[j * count : (j + 1) * count]:
            total = total + ref[...].astype(F32)
        out_ref[j] = total.astype(BF16)


def sum_parts(index, residual, parts):
    per, dec_len, _ = residual.shape
    cols = parts[0].shape[1]
    return pl.pallas_call(
        sum_kernel,
        grid_spec=pltpu.PrefetchScalarGridSpec(
            num_scalar_prefetch=1,
            grid=(1,),
            in_specs=[pl.BlockSpec((per, dec_len, cols), lambda i, s: (0, 0, s[0]))]
            + [full_spec()] * len(parts),
            out_specs=pl.BlockSpec((per, dec_len, cols), lambda i, s: (0, 0, 0)),
        ),
        out_shape=jax.ShapeDtypeStruct((per, dec_len, cols), BF16),
        cost_estimate=cost(per * dec_len * cols * 8, per * dec_len * cols * 12),
        compiler_params=pltpu.CompilerParams(vmem_limit_bytes=8 << 20),
        name="sum_parts",
    )(index, residual, *parts)


def load_kernel(cuts, step, src, *refs):
    dests, sems = refs[:-1], refs[-1]
    copies = []
    for a, b, dest in zip(cuts, cuts[1:], dests):
        for low in range(a, b, step):
            size = min(step, b - low)
            copies.append(
                pltpu.make_async_copy(
                    src.at[pl.ds(low, size)], dest.at[pl.ds(low - a, size)], sems.at[len(copies)]
                )
            )
    for copy in copies:
        copy.start()
    for copy in copies:
        copy.wait()


def load(array, cuts, step, limit):
    shapes = [(b - a,) + array.shape[1:] for a, b in zip(cuts, cuts[1:])]
    count = sum(-(-(b - a) // step) for a, b in zip(cuts, cuts[1:]))
    return pl.pallas_call(
        functools.partial(load_kernel, cuts, step),
        in_specs=[pl.BlockSpec(memory_space=pl.ANY)],
        out_specs=[full_spec()] * len(shapes),
        out_shape=[jax.ShapeDtypeStruct(s, BF16) for s in shapes],
        scratch_shapes=[pltpu.SemaphoreType.DMA((count,))],
        cost_estimate=cost(7e9, 2 * array.size),
        compiler_params=pltpu.CompilerParams(vmem_limit_bytes=limit),
    )(array)


def split3(x):
    hi = x.astype(BF16)
    rest = x - hi.astype(F32)
    mid = rest.astype(BF16)
    low = (rest - mid.astype(F32)).astype(BF16)
    return hi, mid, low


def fill_table(question_ref, table, n_pass, per, n_set):
    chips = n_pass // 2
    me_set, me_seq = lax.axis_index("qset"), lax.axis_index("seq")
    chip = lax.div(me_seq, 2)
    core = me_seq - 2 * chip
    for t in range(n_set * per):
        table[1, t] = -1
        table[2, t] = -1
    for i in range(n_pass):
        hop, flip = divmod(i, 2)
        source = 2 * lax.rem(chip + chips - hop, chips) + (1 - core if flip else core)
        question = question_ref[me_set, source]
        owner = lax.div(question, per)
        number = question - owner * per
        table[0, i] = lax.rem(me_set + n_set - owner, n_set) * per + number
        t = lax.rem(owner + n_set - me_set, n_set) * per + number
        row = jnp.where(table[1, t] < 0, 1, 2)
        table[row, t] = i


def attend_kernel(n_pass, plen, heads, dests, question_ref, *refs):
    q_refs = refs[:dests]
    kv_ref = refs[dests]
    out_refs = refs[dests + 1 : -9]
    qs, score_s, weight_s, part, peak_s, total_s, stat_s, sent_s, table = refs[-9:]
    dec_len, cols = out_refs[0].shape[0], heads * HD
    per = len(out_refs) // dests
    fill_table(question_ref, table, n_pass, per, dests)
    wide = score_s.shape[1] // dec_len
    span_w = wide * HD
    groups = cols // span_w
    for i, ref in enumerate(q_refs):
        for j in range(per):
            qs[i * per + j] = ref[j * dec_len : (j + 1) * dec_len, :]
    head_of = lax.broadcasted_iota(jnp.int32, (dec_len, span_w), 1) // HD
    lane = lax.broadcasted_iota(jnp.int32, (dec_len, LANES), 1)
    units = [(p, g) for p in range(n_pass) for g in range(groups)]

    def pick(stacked):
        kept = stacked[:dec_len]
        for h in range(1, wide):
            kept = jnp.where(head_of == h, stacked[h * dec_len : (h + 1) * dec_len], kept)
        return kept

    for p, g in units:
        span = slice(g * span_w, (g + 1) * span_w)
        q = qs[table[0, p], :, span]
        zero = jnp.zeros_like(q)
        stacked = jnp.concatenate([jnp.where(head_of == h, q, zero) for h in range(wide)], axis=0)
        score_s[p * groups + g] = lax.dot_general(
            stacked,
            kv_ref[0, p * plen : (p + 1) * plen, span],
            (((1,), (1,)), ((), ())),
            preferred_element_type=F32,
        )
    for p in range(n_pass):
        peaks = jnp.zeros((dec_len, LANES), F32)
        totals = jnp.zeros((dec_len, LANES), F32)
        for g in range(groups):
            u = p * groups + g
            scores = score_s[u]
            peak = jnp.max(scores, axis=-1, keepdims=True)
            weights = jnp.exp(scores - peak)
            total = jnp.sum(weights, axis=-1, keepdims=True)
            weight_s[u] = weights.astype(BF16)
            span = slice(g * span_w, (g + 1) * span_w)
            peak_s[p, :, span] = pick(jnp.broadcast_to(peak, (peak.shape[0], span_w)))
            total_s[p, :, span] = pick(jnp.broadcast_to(total, (total.shape[0], span_w)))
            for h in range(wide):
                here = lane == g * wide + h
                rows = slice(h * dec_len, (h + 1) * dec_len)
                peaks = jnp.where(here, peak[rows], peaks)
                totals = jnp.where(here, total[rows], totals)
        stat_s[p, 0] = peaks
        stat_s[p, 1] = totals
    for p, g in units:
        span = slice(g * span_w, (g + 1) * span_w)
        summed = jnp.dot(
            weight_s[p * groups + g],
            kv_ref[1, p * plen : (p + 1) * plen, span],
            preferred_element_type=F32,
        )
        part[p, :, span] = pick(summed)

    for t, out in enumerate(out_refs):
        a, b = table[1, t], table[2, t]

        @pl.when(a < 0)
        def _():
            out[:, :cols] = jnp.zeros((dec_len, cols), BF16)
            sent_s[t, 0] = jnp.full((dec_len, LANES), EMPTY, F32)
            sent_s[t, 1] = jnp.zeros((dec_len, LANES), F32)

        @pl.when((a >= 0) & (b < 0))
        def _():
            out[:, :cols] = (part[a] / total_s[a]).astype(BF16)
            sent_s[t] = stat_s[a]

        @pl.when((a >= 0) & (b >= 0))
        def _():
            top = jnp.maximum(peak_s[a], peak_s[b])
            f_a, f_b = jnp.exp(peak_s[a] - top), jnp.exp(peak_s[b] - top)
            whole = total_s[a] * f_a + total_s[b] * f_b
            out[:, :cols] = ((part[a] * f_a + part[b] * f_b) / whole).astype(BF16)
            peaks = jnp.maximum(stat_s[a, 0], stat_s[b, 0])
            sent_s[t, 0] = peaks
            sent_s[t, 1] = stat_s[a, 1] * jnp.exp(stat_s[a, 0] - peaks) + stat_s[b, 1] * jnp.exp(
                stat_s[b, 0] - peaks
            )

    for r in range(dests):
        pieces = []
        for t in range(r * per, (r + 1) * per):
            for piece in (*split3(sent_s[t, 0]), sent_s[t, 1].astype(BF16)):
                pieces.append(piece[:, :heads])
        room = out_refs[r * per].shape[1] - cols - 4 * heads * per
        if room:
            pieces.append(jnp.zeros((dec_len, room), BF16))
        out_refs[r * per][:, cols:] = jnp.concatenate(pieces, axis=1)


def attend(questions, queries, kv, n_pass, plen, per, dec_len):
    dests = len(queries)
    cols = queries[0].shape[1]
    heads = cols // HD
    rows = n_pass * dec_len
    wide = min(heads, 4)
    units = n_pass * heads // wide
    extra = -(-4 * heads * per // LANES) * LANES
    return pl.pallas_call(
        functools.partial(attend_kernel, n_pass, plen, heads, dests),
        in_specs=[pl.BlockSpec(memory_space=pltpu.SMEM)] + [full_spec()] * (dests + 1),
        out_specs=[full_spec()] * (dests * per),
        out_shape=[
            jax.ShapeDtypeStruct((dec_len, cols if t % per else cols + extra), BF16)
            for t in range(dests * per)
        ],
        scratch_shapes=[
            pltpu.VMEM((dests * per, dec_len, cols), BF16),
            pltpu.VMEM((units, wide * dec_len, plen), F32),
            pltpu.VMEM((units, wide * dec_len, plen), BF16),
            pltpu.VMEM((n_pass, dec_len, cols), F32),
            pltpu.VMEM((n_pass, dec_len, cols), F32),
            pltpu.VMEM((n_pass, dec_len, cols), F32),
            pltpu.VMEM((n_pass, 2, dec_len, LANES), F32),
            pltpu.VMEM((dests * per, 2, dec_len, LANES), F32),
            pltpu.SMEM((3, max(n_pass, dests * per)), jnp.int32),
        ],
        cost_estimate=cost(8 * rows * plen * cols, n_pass * plen * cols * 4),
        compiler_params=pltpu.CompilerParams(vmem_limit_bytes=20 << 20),
        name="attend",
    )(questions, *queries, kv)


def project_kernel(heads, parts, number, chips, blocks, *refs):
    part_refs, stat_refs = refs[:parts], refs[parts : 2 * parts]
    w_ref = refs[2 * parts]
    out_refs, rows_ref = refs[2 * parts + 1 : -1], refs[-1]
    dec_len, cols = part_refs[0].shape[0], heads * HD
    stats = jnp.concatenate([ref[:, cols:] for ref in stat_refs], axis=0)
    row = lax.broadcasted_iota(jnp.int32, (stats.shape[1], cols), 0) - number * 4 * heads
    head = lax.broadcasted_iota(jnp.int32, (stats.shape[1], cols), 1) // HD
    is_peak = functools.reduce(jnp.logical_or, [row == head + i * heads for i in range(3)])
    spread_peak = is_peak.astype(F32).astype(BF16)
    spread_total = (row == head + 3 * heads).astype(F32).astype(BF16)
    peaks = jnp.dot(stats, spread_peak, preferred_element_type=F32)
    totals = jnp.dot(stats, spread_total, preferred_element_type=F32)
    peaks = [peaks[i * dec_len : (i + 1) * dec_len] for i in range(parts)]
    totals = [totals[i * dec_len : (i + 1) * dec_len] for i in range(parts)]
    top = functools.reduce(jnp.maximum, peaks)
    sizes = [t * jnp.exp(p - top) for p, t in zip(peaks, totals)]
    mixed = functools.reduce(
        jnp.add, [ref[:, :cols].astype(F32) * s for ref, s in zip(part_refs, sizes)]
    )
    rows_ref[...] = (mixed / functools.reduce(jnp.add, sizes)).astype(BF16)
    piece = out_refs[0].shape[1]
    me_seq = lax.axis_index("seq")
    chip = lax.div(me_seq, 2)
    core = me_seq - 2 * chip
    for block, out in zip(blocks, out_refs):
        hop, flip = divmod(block, 2)
        dest = 2 * lax.rem(chip + hop, chips) + (1 - core if flip else core)
        cut = pl.ds(pl.multiple_of(dest * piece, piece), piece)
        out[...] = jnp.dot(rows_ref[...], w_ref[:, cut], preferred_element_type=F32).astype(BF16)


def project(number, partials, stats, weight, count, blocks):
    parts = len(partials)
    rows = partials[0].shape[0]
    cols = weight.shape[0]
    piece = weight.shape[1] // count
    return pl.pallas_call(
        functools.partial(project_kernel, cols // HD, parts, number, count // 2, blocks),
        in_specs=[full_spec()] * (2 * parts + 1),
        out_specs=[full_spec()] * len(blocks),
        out_shape=[jax.ShapeDtypeStruct((rows, piece), BF16)] * len(blocks),
        scratch_shapes=[pltpu.VMEM((rows, cols), BF16)],
        cost_estimate=cost(2 * rows * cols * piece * len(blocks), cols * piece * len(blocks) * 2),
        compiler_params=pltpu.CompilerParams(vmem_limit_bytes=16 << 20),
        name="project",
    )(*partials, *stats, weight)


def body(
    states, enc_gain, dec_states, dec_gain, query_weight, key_value_weight, out_weight, question_of
):
    width = states.shape[-1]
    plen = states.shape[2]
    n_set = lax.axis_size("qset")
    n_seq = lax.axis_size("seq")
    me_seq = lax.axis_index("seq")
    per, dec_len = dec_states.shape[0], dec_states.shape[1]
    chips = n_seq // 2
    cuts = [width * c // 16 for c in CUTS]

    def seq_move(hop, flip):
        return [(s, 2 * ((s // 2 + hop) % chips) + ((s % 2) ^ flip)) for s in range(n_seq)]

    def set_move(hop):
        return [(s, (s + hop) % n_set) for s in range(n_set)]

    def cross(own):
        return [lax.ppermute(own, "seq", seq_move(hop, 0)) for hop in range(1, chips)]

    def sibling(rows):
        return lax.ppermute(rows, "seq", seq_move(0, 1))

    own = list(enc_norm(states[0, 0], enc_gain, cuts))
    queries = query_rows(dec_states.reshape(per * dec_len, width), dec_gain, query_weight)
    crossed = [cross(rows) for rows in own]
    all_queries = [queries] + [
        lax.ppermute(queries, "qset", set_move(hop)) for hop in range(1, n_set)
    ]

    kv_parts = load(key_value_weight, cuts, 256, 28 << 20)
    acc = None
    for c, weight in enumerate(kv_parts):
        beside, here = sibling(own[c]), crossed[c]
        forwarded = [sibling(rows) for rows in here]
        chunks = [own[c], beside]
        for pair in zip(here, forwarded):
            chunks += pair
        part = jnp.einsum(
            "rd,dkc->rkc", jnp.concatenate(chunks, axis=0), weight, preferred_element_type=F32
        )
        acc = part if acc is None else acc + part
    kv = jnp.transpose(acc.astype(BF16), (1, 0, 2))

    sent = list(attend(question_of[:, :, 0], all_queries, kv, n_seq, plen, per, dec_len))
    out_source, sent[0] = lax.optimization_barrier((out_weight, sent[0]))
    (out_part,) = load(out_source, [0, out_weight.shape[0]], 256, 44 << 20)
    moves = [(hop, f) for hop in range(chips) for f in range(2)]

    partials = []
    for j in range(per):
        partials.append(
            [sent[j]]
            + [lax.ppermute(sent[hop * per + j], "qset", set_move(hop)) for hop in range(1, n_set)]
        )
    parts = []
    for j in range(per):
        for blocks in (list(range(2, n_seq)), [0, 1]):
            out = project(j, partials[j], partials[0], out_part, n_seq, blocks)
            parts += [
                lax.ppermute(rows, "seq", seq_move(*moves[k])) if k else rows
                for k, rows in zip(blocks, out)
            ]
    return sum_parts(me_seq.reshape(1).astype(jnp.int32), dec_states, parts)


def solution(mesh):
    return jax.shard_map(
        body,
        mesh=mesh,
        in_specs=(
            P(("groups", "qset"), "seq", None, None),
            P(),
            P(("groups", "qset"), None, None),
            P(),
            P(None, "seq"),
            P(None, None, "seq"),
            P("seq", None),
            P("groups", None, None),
        ),
        out_specs=P(("groups", "qset"), None, "seq"),
        check_vma=False,
    )
```
